256 devices in a mesh: bank: 16 (over z, core), zero: 16 (over y, x).
Axes of the slice: x: 4, y: 4, z: 8, core: 2. Of those that a mesh axis runs over, the one named last changes fastest.
Arguments:
- master_down: float32 [64, 1024, 2048], P('bank', None, 'zero'), may hold values from -0.25 to 0.25
- second_down: bfloat16 [64, 1024, 2048], P('bank', None, 'zero'), may hold values from -0.09375 to 0.09375
- router_weight: float32 [2048, 64], P('zero', 'bank'), may hold values from -0.125 to 0.125
- router_gain: float32 [2048], P('zero'), may hold values from 0.25 to 1.75
Outputs:
- final_down: bfloat16 [64, 1024, 2048], P('bank')
- scale_down: float32 [64, 1024], P('bank')
- serve_router: bfloat16 [2048, 64], replicated
The draws below stay inside these ranges and needn't reach their ends.
All inputs are finite; a program needn't handle non-finite values. Where the reference program divides by a largest or mean magnitude, that divisor is 1e-20 or more.
Results may differ from the reference program's by a relative error of at most 0.001.
Values may be sent and summed in bfloat16 or wider, within the bound.
A program may use at most 128 MiB of HBM per device.

```python
import jax
import jax.numpy as jnp

EXPERTS = 64
D_MODEL = 2048
D_EXPERT = 1024


def with_spikes(values, own_key, source, target, shards_of, factor):
    def block_of(position):
        return (jnp.arange(values.shape[position]) // (values.shape[position] // shards_of)).reshape((-1,) + (1,) * (values.ndim - 1 - position))

    near = jax.random.permutation(own_key, shards_of)[block_of(target)]
    second = (block_of(target) + shards_of // 2) % shards_of
    return jnp.where((block_of(source) == near) | (block_of(source) == second), factor * values, values)


def steps_of(stream_key, extent, cuts, least, top_value):
    factor_of, own = 1.0, jax.random.fold_in(stream_key, 6)
    for axis_at, parts in cuts:
        draws = jnp.exp(jax.random.uniform(jax.random.fold_in(own, axis_at), (parts,), jnp.float32, least / len(cuts), top_value / len(cuts)))
        factor_of = factor_of * jnp.repeat(draws, extent[axis_at] // parts).reshape([-1 if axis == axis_at else 1 for axis in range(len(extent))])
    return factor_of


def bell_draw(stream_key, shape, deviation, reach, split=(), dtype=jnp.bfloat16):
    factor_of = steps_of(stream_key, shape, split, -0.22, 0.18) if split else 1.0
    entries = jax.random.normal(stream_key, shape, jnp.float32) * deviation * factor_of
    return jnp.minimum(jnp.maximum(entries, -reach), reach).astype(dtype)


def noise_with(key, dims, width, bound, split, heavy, kind=jnp.bfloat16):
    entries = width * jax.random.normal(key, dims, jnp.float32)
    if split:
        entries = entries * steps_of(key, dims, split, -0.22, 0.18)
    return jnp.clip(with_spikes(entries, jax.random.fold_in(key, 3), *heavy), -bound, bound).astype(kind)


def setup_inputs(seed: int = 0) -> dict:
    key_of = jax.random.split(jax.random.key(seed), 5)
    master_down = noise_with(key_of[0], (EXPERTS, D_EXPERT, D_MODEL), D_EXPERT ** -0.5, 0.25, ((0, 16), (2, 16)), (2, 1, 16, 2.0), jnp.float32)
    second_down = bell_draw(key_of[1], (EXPERTS, D_EXPERT, D_MODEL), (D_EXPERT * 4) ** -0.5, 0.09375, ((0, 16), (2, 16)))
    router_weight = bell_draw(key_of[2], (D_MODEL, EXPERTS), D_MODEL ** -0.5, 0.125, ((0, 16), (1, 16)), jnp.float32)
    router_gain = jnp.clip(1.0 + 0.15 * jax.random.normal(key_of[3], (D_MODEL,), jnp.float32), 0.25, 1.75)
    return {"master_down": master_down, "second_down": second_down, "router_weight": router_weight, "router_gain": router_gain}


def reference(master_down, second_down, router_weight, router_gain):
    merged_down = master_down + second_down.astype(jnp.float32)
    scale_down = jnp.max(jnp.abs(merged_down), axis=2)
    final_down = (merged_down / jnp.expand_dims(scale_down, 2)).astype(jnp.bfloat16)
    serve_router = (router_weight * router_gain[:, None]).astype(jnp.bfloat16)
    return final_down, scale_down, serve_router
```

```python
import jax
import jax.numpy as jnp
from jax import lax
from jax.experimental import pallas as pl
from jax.experimental.pallas import tpu as pltpu
from jax.sharding import PartitionSpec as P

SIDE = 4
PLANE = SIDE * SIDE
PIECES = 8
LEAD = 3
MESH = pl.DeviceIdType.MESH
F32 = jnp.float32
BF16 = jnp.bfloat16


def routes(piece, origin, via):
    turned, half = piece % 2, (piece // 2) % 2
    first, second = origin if not turned else origin[::-1]
    if via is None:
        legs = [(0, 3), (1, 3), (2, 1 - half), (3, half)]
    else:
        along = via ^ (2 * turned)
        if along < 2:
            legs = [(2, 1 - half), (3, half)]
            if (along, first, half) in ((0, SIDE - 1, 0), (1, 1, 1)):
                legs.append((along, 2))
        elif (along, second, half) in ((2, SIDE - 1, 0), (3, 1, 1)):
            legs = [(along, 0)]
        else:
            legs = []
    return [(direction ^ (2 * turned), weight) for direction, weight in legs]


STEP = ((-1, 0), (1, 0), (0, -1), (0, 1))


def schedule():
    waiting = [[] for _ in range(4)]
    order = [[] for _ in range(4)]
    for piece in range(PIECES):
        for direction, weight in routes(piece, (0, 0), None):
            waiting[direction].append((-weight, 0, piece, (0, 0)))

    def pick():
        for direction in range(4):
            if waiting[direction]:
                best = min(waiting[direction])
                waiting[direction].remove(best)
                order[direction].append(best[2:])

    for _ in range(LEAD):
        pick()
    for turn in range((PLANE - 1) * PIECES // 4):
        for direction in range(4):
            piece, origin = order[direction][turn]
            origin = tuple((o + s) % SIDE for o, s in zip(origin, STEP[direction]))
            for onward, weight in routes(piece, origin, direction):
                waiting[onward].append((-weight, turn + 1, piece, origin))
        pick()
    return order


ORDER = schedule()
TURNS = (PLANE - 1) * PIECES // 4
assert all(len(lane) == TURNS for lane in ORDER)


def exchange(
    master, second, weight, gain, slab, scale_out, router_out,
    merged, change, weight_in, gain_in, tops, inverse, columns, banks, wide,
    load_sem, tops_send, tops_recv, send_sem, recv_sem, ring_send, ring_recv, pair_send, pair_recv,
):
    experts, rows, lanes = master.shape
    per_piece = experts * rows // PIECES
    bank_count = banks.shape[0]
    me = lax.axis_index("zero")
    bank = lax.axis_index("bank")
    my_x, my_y = lax.rem(me, SIDE), lax.div(me, SIDE)

    def at(x, y):
        return lax.rem(my_y + y, SIDE) * SIDE + lax.rem(my_x + x, SIDE)

    neighbour = (at(1, 0), at(SIDE - 1, 0), at(0, 1), at(0, SIDE - 1))
    above = lax.rem(bank + 2, bank_count)
    below = lax.rem(bank + bank_count - 2, bank_count)
    partner = bank + 1 - 2 * lax.rem(bank, 2)

    loads = []
    for e in range(experts):
        loads.append(
            (
                pltpu.make_async_copy(master.at[e], merged.at[e], load_sem.at[2 * e]),
                pltpu.make_async_copy(second.at[e], change.at[e], load_sem.at[2 * e + 1]),
            )
        )
        for load in loads[-1]:
            load.start()
    small = (
        pltpu.make_async_copy(weight, weight_in, load_sem.at[2 * experts]),
        pltpu.make_async_copy(gain, gain_in, load_sem.at[2 * experts + 1]),
    )
    for load in small:
        load.start()

    barrier = pltpu.get_barrier_semaphore()
    others = [at(x, y) for y in range(SIDE) for x in range(SIDE) if (x, y) != (0, 0)]
    for other in others:
        pl.semaphore_signal(barrier, inc=1, device_id={"zero": other}, device_id_type=MESH)
    for other in (above, below, partner):
        pl.semaphore_signal(barrier, inc=1, device_id={"bank": other}, device_id_type=MESH)

    lane = lax.broadcasted_iota(jnp.int32, (8, lanes), 1)
    groups = rows // 16

    def find_tops(e):
        for load in loads[e]:
            load.wait()

        def body(g, top):
            at_rows = pl.ds(pl.multiple_of(g * 16, 16), 16)
            total = merged[e, at_rows, :] + change[e, at_rows, :].astype(F32)
            merged[e, at_rows, :] = total
            peak = jnp.max(jnp.abs(total), axis=1, keepdims=True)
            top = jnp.where(lane == 2 * g, peak[:8], top)
            return jnp.where(lane == 2 * g + 1, peak[8:], top)

        tops[me, e] = lax.fori_loop(0, groups, body, jnp.zeros((8, lanes), F32), unroll=8)

    def share_tops(first, last, message):
        sends = []
        for i, other in enumerate(others):
            part = tops.at[me, pl.ds(first, last - first)]
            sends.append(
                pltpu.make_async_remote_copy(
                    part, part, tops_send.at[message, i], tops_recv.at[message, i],
                    device_id={"zero": other}, device_id_type=MESH,
                )
            )
            sends[-1].start()
        return sends

    def divide(e):
        top = jnp.max(tops[:, e], axis=0)
        columns[e] = top
        inverse[...] = 1.0 / top

        def body(g, carry):
            here = pltpu.roll(inverse[...], lax.rem(lanes - 8 * g, lanes), 1)
            for i in range(4):
                at_rows = pl.ds(pl.multiple_of(g * 64 + 16 * i, 16), 16)
                low = jnp.broadcast_to(here[:, 2 * i : 2 * i + 1], (8, lanes))
                high = jnp.broadcast_to(here[:, 2 * i + 1 : 2 * i + 2], (8, lanes))
                value = merged[e, at_rows, :] * jnp.concatenate([low, high], axis=0)
                to_rows = pl.ds(pl.multiple_of(e * rows + g * 64 + 16 * i, 16), 16)
                slab[me, to_rows, :] = value.astype(BF16)
            return carry

        lax.fori_loop(0, groups // 4, body, 0, unroll=2)

    find_tops(0)
    pl.semaphore_wait(barrier, PLANE - 1 + 3)
    top_sends = share_tops(0, 1, 0)
    for e in range(1, experts):
        find_tops(e)
    for load in small:
        load.wait()
    tops[me, experts, 0:4, :] = weight_in[...] * gain_in[...]
    tops[me, experts, 4:8, :] = jnp.zeros((4, lanes), F32)
    late_sends = share_tops(1, experts + 1, 1)

    in_flight = []

    def send(direction, turn):
        piece, (x, y) = ORDER[direction][turn]
        part = slab.at[at(x, y), pl.ds(piece * per_piece, per_piece)]
        copy = pltpu.make_async_remote_copy(
            part, part, send_sem.at[direction, turn], recv_sem.at[direction, turn],
            device_id={"zero": neighbour[direction]}, device_id_type=MESH,
        )
        copy.start()
        in_flight.append(copy)

    def receive(direction, turn):
        piece, origin = ORDER[direction][turn]
        x, y = (o + s for o, s in zip(origin, STEP[direction]))
        part = slab.at[at(x + SIDE, y + SIDE), pl.ds(piece * per_piece, per_piece)]
        pltpu.make_async_remote_copy(
            part, part, send_sem.at[direction, turn], recv_sem.at[direction, turn],
            device_id={"zero": neighbour[direction]}, device_id_type=MESH,
        ).wait_recv()

    done = 0

    def ready(upto):
        nonlocal done
        while done < min(upto, experts):
            if done < 2:
                for copy in (top_sends, late_sends)[done]:
                    copy.wait_recv()
            divide(done)
            done += 1

    for turn in range(LEAD):
        needed = max(ORDER[d][turn][0] for d in range(4) if ORDER[d][turn][1] == (0, 0))
        ready(needed * per_piece // rows + 1)
        for direction in range(4):
            send(direction, turn)
    ready(experts)

    ring_copies, pair_copies = [], []

    def own_bank():
        for j in range(PLANE):
            banks[bank, :, lanes * j : lanes * (j + 1)] = tops[j, experts, 0:4, :]

    def bank_at(shift):
        return lax.rem(bank + bank_count + shift, bank_count)

    def ring(step):
        for way, shift, other in ((0, -2, above), (1, 2, below)):
            if step > (4 if way == 0 else 3):
                continue
            part = banks.at[bank_at(shift * (step - 1))]
            copy = pltpu.make_async_remote_copy(
                part, part, ring_send.at[way, step - 1], ring_recv.at[way, step - 1],
                device_id={"bank": other}, device_id_type=MESH,
            )
            copy.start()
            ring_copies.append(copy)

    def ring_arrived(step):
        for copy in ring_copies[2 * (step - 1) : 2 * step]:
            copy.wait_recv()

    def pair(step):
        shifts = (0,) if step == 0 else (-2 * step, 2 * step) if step < 4 else (-2 * step,)
        for shift in shifts:
            part = banks.at[bank_at(shift)]
            n = len(pair_copies)
            copy = pltpu.make_async_remote_copy(
                part, part, pair_send.at[n], pair_recv.at[n],
                device_id={"bank": partner}, device_id_type=MESH,
            )
            copy.start()
            pair_copies.append(copy)

    def finish_scale():
        for e in range(experts):
            wide[0:lanes, 0:8] = jnp.transpose(columns[e])
            line = jnp.zeros((8, lanes), F32)
            for q in range(16):
                part = wide[pl.ds(q, 8, stride=16), 0:lanes]
                part = pltpu.roll(part, 8 * q, 1) if q else part
                line = jnp.where((lane >= 8 * q) & (lane < 8 * q + 8), part, line)
            for r in range(8):
                scale_out[e : e + 1, lanes * r : lanes * (r + 1)] = line[r : r + 1, :]

    def finish_router():
        for copy in pair_copies:
            copy.wait_recv()
        for b in range(bank_count):
            router_out[4 * b : 4 * b + 4, :] = banks[b]

    def ring_step(step):
        def run():
            ring_arrived(step)
            if step < 4:
                ring(step + 1)
            pair(step)

        return run

    def first_step():
        own_bank()
        ring(1)
        pair(0)

    every = TURNS // 10
    extras = {
        1: finish_scale,
        every: first_step,
        2 * every: ring_step(1),
        3 * every: ring_step(2),
        4 * every: ring_step(3),
        5 * every: ring_step(4),
        6 * every: finish_router,
    }

    for turn in range(TURNS):
        for direction in range(4):
            receive(direction, turn)
        if turn + LEAD < TURNS:
            for direction in range(4):
                send(direction, turn + LEAD)
        if turn in extras:
            extras[turn]()
    for copy in in_flight + top_sends + late_sends + ring_copies + pair_copies:
        copy.wait_send()


def store(slab, scale_in, router_in, final, scale, router, half, sem):
    experts, rows, width = final.shape
    lanes = width // PLANE
    copies = []
    for e in range(experts):
        for j in range(PLANE):
            copies.append(
                pltpu.make_async_copy(
                    slab.at[j, pl.ds(e * rows, rows)],
                    final.at[e, :, pl.ds(j * lanes, lanes)],
                    sem.at[e * PLANE + j],
                )
            )
    for copy in copies:
        copy.start()
    half[...] = router_in[...].astype(BF16)
    copies.append(pltpu.make_async_copy(scale_in, scale, sem.at[experts * PLANE]))
    copies.append(pltpu.make_async_copy(half, router, sem.at[experts * PLANE + 1]))
    copies[-2].start()
    copies[-1].start()
    for copy in copies:
        copy.wait()


def shards(master, second, weight, gain):
    experts, rows, lanes = master.shape
    banks = lax.axis_size("bank")
    width = lanes * PLANE
    hbm = pl.BlockSpec(memory_space=pltpu.HBM)
    vmem = pl.BlockSpec(memory_space=pltpu.VMEM)
    dma = pltpu.SemaphoreType.DMA
    values = (master, second, weight.T, gain.reshape(1, lanes))
    slab, scale, router = pl.pallas_call(
        exchange,
        out_shape=(
            pltpu.VMEM((PLANE, experts * rows, lanes), BF16),
            pltpu.VMEM((experts, rows), F32),
            pltpu.VMEM((banks * experts, width), F32),
        ),
        in_specs=[hbm] * 4,
        out_specs=(vmem,) * 3,
        scratch_shapes=[
            pltpu.VMEM((experts, rows, lanes), F32),
            pltpu.VMEM((experts, rows, lanes), BF16),
            pltpu.VMEM((experts, lanes), F32),
            pltpu.VMEM((1, lanes), F32),
            pltpu.VMEM((PLANE, experts + 1, 8, lanes), F32),
            pltpu.VMEM((8, lanes), F32),
            pltpu.VMEM((experts, 8, lanes), F32),
            pltpu.VMEM((banks, experts, width), F32),
            pltpu.VMEM((lanes, lanes), F32),
            dma((2 * experts + 2,)),
            dma((2, PLANE - 1)),
            dma((2, PLANE - 1)),
            dma((4, TURNS)),
            dma((4, TURNS)),
            dma((2, 4)),
            dma((2, 4)),
            dma((8,)),
            dma((8,)),
        ],
        compiler_params=pltpu.CompilerParams(
            collective_id=0, has_side_effects=True, vmem_limit_bytes=24 << 20
        ),
        name="exchange",
    )(*(pltpu.with_memory_space_constraint(value, pltpu.HBM) for value in values))
    final, scale, router = pl.pallas_call(
        store,
        out_shape=(
            jax.ShapeDtypeStruct((experts, rows, width), BF16),
            jax.ShapeDtypeStruct((experts, rows), F32),
            jax.ShapeDtypeStruct((banks * experts, width), BF16),
        ),
        in_specs=[vmem] * 3,
        out_specs=(hbm,) * 3,
        scratch_shapes=[
            pltpu.VMEM((banks * experts, width), BF16),
            dma((experts * PLANE + 2,)),
        ],
        compiler_params=pltpu.CompilerParams(vmem_limit_bytes=4 << 20),
        name="store",
    )(slab, scale, router)
    return final, scale, router.T


def solution(mesh):
    return jax.shard_map(
        shards,
        mesh=mesh,
        in_specs=(P("bank", None, "zero"), P("bank", None, "zero"), P("zero", "bank"), P("zero")),
        out_specs=(P("bank", None, None), P("bank", None), P()),
        check_vma=False,
    )
```

```python
import jax
import jax.numpy as jnp
from jax import lax
from jax.experimental import pallas as pl
from jax.experimental.pallas import tpu as pltpu
from jax.sharding import PartitionSpec as P

SIDE = 4
PLANE = SIDE * SIDE
EXPERTS = 4
PIECES = 8
LEAD = 4
MESH = pl.DeviceIdType.MESH
F32 = jnp.float32
BF16 = jnp.bfloat16


def routes(piece, origin, via):
    turned, half = piece % 2, (piece // 2) % 2
    first, second = origin if not turned else origin[::-1]
    if via is None:
        legs = [(0, 3), (1, 3), (2, 1 - half), (3, half)]
    else:
        along = via ^ (2 * turned)
        if along < 2:
            legs = [(2, 1 - half), (3, half)]
            if (along, first, half) in ((0, SIDE - 1, 0), (1, 1, 1)):
                legs.append((along, 2))
        elif (along, second, half) in ((2, SIDE - 1, 0), (3, 1, 1)):
            legs = [(along, 0)]
        else:
            legs = []
    return [(direction ^ (2 * turned), weight) for direction, weight in legs]


STEP = ((-1, 0), (1, 0), (0, -1), (0, 1))


def schedule():
    waiting = [[] for _ in range(4)]
    order = [[] for _ in range(4)]
    for piece in range(PIECES):
        for direction, weight in routes(piece, (0, 0), None):
            waiting[direction].append((-weight, 0, piece, (0, 0)))

    def pick():
        for direction in range(4):
            limit = (len(order[direction]) // 2 + 1) * PIECES // EXPERTS
            now = [entry for entry in waiting[direction] if entry[2] < limit or entry[1]]
            if now:
                best = min(now)
                waiting[direction].remove(best)
                order[direction].append(best[2:])

    for _ in range(LEAD):
        pick()
    for turn in range((PLANE - 1) * PIECES // 4):
        for direction in range(4):
            piece, origin = order[direction][turn]
            origin = tuple((o + s) % SIDE for o, s in zip(origin, STEP[direction]))
            for onward, weight in routes(piece, origin, direction):
                waiting[onward].append((-weight, turn + 1, piece, origin))
        pick()
    return order


ORDER = schedule()
TURNS = (PLANE - 1) * PIECES // 4
assert all(len(lane) == TURNS for lane in ORDER)


def exchange(
    master, second, weight, gain, slab, scale_out, router_out,
    merged, change, weight_in, gain_in, tops, part_router, inverse, columns, banks, wide,
    load_sem, tops_send, tops_recv, hello, send_sem, recv_sem, ring_send, ring_recv, pair_send, pair_recv,
):
    experts, rows, lanes = master.shape
    per_piece = experts * rows // PIECES
    bank_count = banks.shape[0]
    me = lax.axis_index("zero")
    bank = lax.axis_index("bank")
    my_x, my_y = lax.rem(me, SIDE), lax.div(me, SIDE)

    def at(x, y):
        return lax.rem(my_y + y, SIDE) * SIDE + lax.rem(my_x + x, SIDE)

    neighbour = (at(1, 0), at(SIDE - 1, 0), at(0, 1), at(0, SIDE - 1))
    above = lax.rem(bank + 2, bank_count)
    below = lax.rem(bank + bank_count - 2, bank_count)
    partner = bank + 1 - 2 * lax.rem(bank, 2)

    loads = []
    for e in range(experts):
        loads.append(
            (
                pltpu.make_async_copy(master.at[e], merged.at[e], load_sem.at[2 * e]),
                pltpu.make_async_copy(second.at[e], change.at[e], load_sem.at[2 * e + 1]),
            )
        )
        for load in loads[-1]:
            load.start()
    small = (
        pltpu.make_async_copy(weight, weight_in, load_sem.at[2 * experts]),
        pltpu.make_async_copy(gain, gain_in, load_sem.at[2 * experts + 1]),
    )
    for load in small:
        load.start()

    barrier = pltpu.get_barrier_semaphore()
    others = [at(x, y) for y in range(SIDE) for x in range(SIDE) if (x, y) != (0, 0)]
    for other in others:
        pl.semaphore_signal(barrier, inc=1, device_id={"zero": other}, device_id_type=MESH)
    floor, core = lax.div(bank, 2), lax.rem(bank, 2)
    last = bank_count // 2 - 1

    def greet(semaphore, condition, other):
        @pl.when(condition)
        def _():
            pl.semaphore_signal(semaphore, inc=1, device_id={"bank": other}, device_id_type=MESH)

    def flag(condition):
        return jnp.where(condition, 1, 0)

    greet(barrier, floor < last, above)
    greet(barrier, floor == 0, below)
    greet(barrier, core == 0, partner)

    lane = lax.broadcasted_iota(jnp.int32, (8, lanes), 1)
    groups = rows // 16

    def find_tops(e):
        for load in loads[e]:
            load.wait()

        def body(g, top):
            at_rows = pl.ds(pl.multiple_of(g * 16, 16), 16)
            total = merged[e, at_rows, :] + change[e, at_rows, :].astype(F32)
            merged[e, at_rows, :] = total
            peak = jnp.max(jnp.abs(total), axis=1, keepdims=True)
            top = jnp.where(lane == 2 * g, peak[:8], top)
            return jnp.where(lane == 2 * g + 1, peak[8:], top)

        return lax.fori_loop(0, groups, body, jnp.zeros((8, lanes), F32), unroll=8)

    def remote(part, send_semaphore, recv_semaphore, other):
        return pltpu.make_async_remote_copy(
            part, part, send_semaphore, recv_semaphore, device_id=other, device_id_type=MESH
        )

    def to_all(values, message):
        for other in others:
            remote(values.at[me], tops_send.at[message], tops_recv.at[message], {"zero": other}).start()

        return remote(
            values.at[pl.ds(0, PLANE - 1)], tops_send.at[message], tops_recv.at[message], {"zero": me}
        )

    def divide(e, top):
        columns[e] = top
        inverse[...] = 1.0 / top

        def body(g, carry):
            here = pltpu.roll(inverse[...], lax.rem(lanes - 8 * g, lanes), 1)
            for i in range(4):
                at_rows = pl.ds(pl.multiple_of(g * 64 + 16 * i, 16), 16)
                low = jnp.broadcast_to(here[:, 2 * i : 2 * i + 1], (8, lanes))
                high = jnp.broadcast_to(here[:, 2 * i + 1 : 2 * i + 2], (8, lanes))
                value = merged[e, at_rows, :] * jnp.concatenate([low, high], axis=0)
                to_rows = pl.ds(pl.multiple_of(e * rows + g * 64 + 16 * i, 16), 16)
                slab[me, to_rows, :] = value.astype(BF16)
            return carry

        lax.fori_loop(0, groups // 4, body, 0, unroll=2)

    shared = []
    for e in range(experts):
        tops[e, me] = find_tops(e)
        if e == 0:
            pl.semaphore_wait(barrier, PLANE - 1 + flag(floor > 0) + flag(floor == last) + core)
        shared.append(to_all(tops.at[e], e))
    for load in small:
        load.wait()
    part_router[me] = weight_in[...] * gain_in[...]
    shared.append(to_all(part_router, experts))

    def send(direction, turn):
        piece, (x, y) = ORDER[direction][turn]
        part = slab.at[at(x, y), pl.ds(piece * per_piece, per_piece)]
        remote(part, send_sem, recv_sem.at[turn], {"zero": neighbour[direction]}).start()

    def receive(turn):
        part = slab.at[0, pl.ds(0, 4 * per_piece)]
        remote(part, send_sem, recv_sem.at[turn], {"zero": me}).wait_recv()

    for e in range(experts):
        shared[e].wait_recv()
        divide(e, jnp.max(tops[e], axis=0))
        for turn in range(2 * e, min(2 * e + 2, LEAD)):
            for direction in range(4):
                send(direction, turn)

    def own_bank():
        for j in range(PLANE):
            banks[bank, :, lanes * j : lanes * (j + 1)] = part_router[j]

    def bank_at(shift):
        return lax.rem(bank + bank_count + shift, bank_count)

    ring_copies = []
    pairs = remote(banks.at[pl.ds(0, bank_count // 2)], pair_send, pair_recv, {"bank": bank})

    def ring(step):
        for way, shift, other in ((0, -2, above), (1, 2, below)):
            if step <= bank_count // 4 - way:
                part = banks.at[bank_at(shift * (step - 1))]
                copy = remote(part, ring_send, ring_recv.at[way, step - 1], {"bank": other})
                copy.start()
                ring_copies.append((step, copy))

    def ring_arrived(step):
        for when, copy in ring_copies:
            if when == step:
                copy.wait_recv()

    def pair(shift):
        remote(banks.at[bank_at(shift)], pair_send, pair_recv, {"bank": partner}).start()

    def finish_scale():
        for e in range(experts):
            wide[0:lanes, 0:8] = jnp.transpose(columns[e])
            line = jnp.zeros((8, lanes), F32)
            for q in range(16):
                part = wide[pl.ds(q, 8, stride=16), 0:lanes]
                part = pltpu.roll(part, 8 * q, 1) if q else part
                line = jnp.where((lane >= 8 * q) & (lane < 8 * q + 8), part, line)
            for r in range(8):
                scale_out[e : e + 1, lanes * r : lanes * (r + 1)] = line[r : r + 1, :]

    def finish_router():
        pairs.wait_recv()
        for b in range(bank_count):
            router_out[4 * b : 4 * b + 4, :] = banks[b]

    def ring_step(step):
        def run():
            ring_arrived(step)
            ring(step + 1)
            pair(-2 * step)
            if step < 4:
                pair(2 * step)

        return run

    def say_hello():
        greet(hello, floor > 0, below)
        greet(hello, floor == last, above)
        greet(hello, core == 1, partner)

    def first_step():
        shared[experts].wait_recv()
        own_bank()
        greeted = flag(floor < last) + flag(floor == 0) + 1 - core

        @pl.when(greeted > 0)
        def _():
            pl.semaphore_wait(hello, greeted)

        ring(1)
        pair(0)

    every = TURNS // 10
    extras = {
        0: say_hello,
        1: finish_scale,
        every: first_step,
        2 * every: ring_step(1),
        3 * every: ring_step(2),
        4 * every: ring_step(3),
        5 * every: ring_step(4),
        6 * every: finish_router,
    }

    for turn in range(TURNS):
        receive(turn)
        if turn + LEAD < TURNS:
            for direction in range(4):
                send(direction, turn + LEAD)
        if turn in extras:
            extras[turn]()
    remote(slab.at[pl.ds(0, PLANE - 1)], send_sem, recv_sem.at[0], {"zero": me}).wait_send()
    for copy in shared:
        copy.wait_send()
    remote(
        banks.at[pl.ds(0, bank_count // 2 - 1)], ring_send, ring_recv.at[0, 0], {"bank": bank}
    ).wait_send()
    pairs.wait_send()


def store(slab, scale_in, router_in, final, scale, router, half, sem):
    experts, rows, width = final.shape
    lanes = width // PLANE
    for e in range(experts):
        for j in range(PLANE):
            pltpu.make_async_copy(
                slab.at[j, pl.ds(e * rows, rows)],
                final.at[e, :, pl.ds(j * lanes, lanes)],
                sem.at[0],
            ).start()
    half[...] = router_in[...].astype(BF16)
    small = (
        pltpu.make_async_copy(scale_in, scale, sem.at[1]),
        pltpu.make_async_copy(half, router, sem.at[2]),
    )
    for copy in small:
        copy.start()
    for copy in small:
        copy.wait()
    pltpu.make_async_copy(slab, slab, sem.at[0]).wait()


def shards(master, second, weight, gain):
    experts, rows, lanes = master.shape
    banks = lax.axis_size("bank")
    width = lanes * PLANE
    hbm = pl.BlockSpec(memory_space=pltpu.HBM)
    vmem = pl.BlockSpec(memory_space=pltpu.VMEM)
    dma = pltpu.SemaphoreType.DMA
    values = (master, second, weight.T, gain.reshape(1, lanes))
    slab, scale, router = pl.pallas_call(
        exchange,
        out_shape=(
            pltpu.VMEM((PLANE, experts * rows, lanes), BF16),
            pltpu.VMEM((experts, rows), F32),
            pltpu.VMEM((banks * experts, width), F32),
        ),
        in_specs=[hbm] * 4,
        out_specs=(vmem,) * 3,
        scratch_shapes=[
            pltpu.VMEM((experts, rows, lanes), F32),
            pltpu.VMEM((experts, rows, lanes), BF16),
            pltpu.VMEM((experts, lanes), F32),
            pltpu.VMEM((1, lanes), F32),
            pltpu.VMEM((experts, PLANE, 8, lanes), F32),
            pltpu.VMEM((PLANE, experts, lanes), F32),
            pltpu.VMEM((8, lanes), F32),
            pltpu.VMEM((experts, 8, lanes), F32),
            pltpu.VMEM((banks, experts, width), F32),
            pltpu.VMEM((lanes, lanes), F32),
            dma((2 * experts + 2,)),
            dma((experts + 1,)),
            dma((experts + 1,)),
            pltpu.SemaphoreType.REGULAR,
            dma,
            dma((TURNS,)),
            dma,
            dma((2, banks // 4)),
            dma,
            dma,
        ],
        compiler_params=pltpu.CompilerParams(
            collective_id=0, has_side_effects=True, vmem_limit_bytes=24 << 20
        ),
        name="exchange",
    )(*(pltpu.with_memory_space_constraint(value, pltpu.HBM) for value in values))
    final, scale, router = pl.pallas_call(
        store,
        out_shape=(
            jax.ShapeDtypeStruct((experts, rows, width), BF16),
            jax.ShapeDtypeStruct((experts, rows), F32),
            jax.ShapeDtypeStruct((banks * experts, width), BF16),
        ),
        in_specs=[vmem] * 3,
        out_specs=(hbm,) * 3,
        scratch_shapes=[
            pltpu.VMEM((banks * experts, width), BF16),
            dma((3,)),
        ],
        compiler_params=pltpu.CompilerParams(vmem_limit_bytes=4 << 20),
        name="store",
    )(slab, scale, router)
    return final, scale, router.T


def solution(mesh):
    return jax.shard_map(
        shards,
        mesh=mesh,
        in_specs=(P("bank", None, "zero"), P("bank", None, "zero"), P("zero", "bank"), P("zero")),
        out_specs=(P("bank", None, None), P("bank", None), P()),
        check_vma=False,
    )
```

```python
import jax
import jax.numpy as jnp
from jax import lax
from jax.experimental import pallas as pl
from jax.experimental.pallas import tpu as pltpu
from jax.sharding import PartitionSpec as P

SIDE = 4
PLANE = SIDE * SIDE
EXPERTS = 4
PIECES = 8
LEAD = 4
MESH = pl.DeviceIdType.MESH
F32 = jnp.float32
BF16 = jnp.bfloat16


def routes(piece, origin, via):
    turned, half = piece % 2, (piece // 2) % 2
    first, second = origin if not turned else origin[::-1]
    if via is None:
        legs = [(0, 3), (1, 3), (2, 1 - half), (3, half)]
    else:
        along = via ^ (2 * turned)
        if along < 2:
            legs = [(2, 1 - half), (3, half)]
            if (along, first, half) in ((0, SIDE - 1, 0), (1, 1, 1)):
                legs.append((along, 2))
        elif (along, second, half) in ((2, SIDE - 1, 0), (3, 1, 1)):
            legs = [(along, 0)]
        else:
            legs = []
    return [(direction ^ (2 * turned), weight) for direction, weight in legs]


STEP = ((-1, 0), (1, 0), (0, -1), (0, 1))


def schedule():
    waiting = [[] for _ in range(4)]
    order = [[] for _ in range(4)]
    for piece in range(PIECES):
        for direction, weight in routes(piece, (0, 0), None):
            waiting[direction].append((-weight, 0, piece, (0, 0)))

    def pick():
        for direction in range(4):
            limit = (len(order[direction]) // 2 + 1) * PIECES // EXPERTS
            now = [entry for entry in waiting[direction] if entry[2] < limit or entry[1]]
            if now:
                best = min(now)
                waiting[direction].remove(best)
                order[direction].append(best[2:])

    for _ in range(LEAD):
        pick()
    for turn in range((PLANE - 1) * PIECES // 4):
        for direction in range(4):
            piece, origin = order[direction][turn]
            origin = tuple((o + s) % SIDE for o, s in zip(origin, STEP[direction]))
            for onward, weight in routes(piece, origin, direction):
                waiting[onward].append((-weight, turn + 1, piece, origin))
        pick()
    return order


ORDER = schedule()
TURNS = (PLANE - 1) * PIECES // 4
assert all(len(lane) == TURNS for lane in ORDER)


def exchange(
    master, second, weight, gain, slab, scale_out, router_out,
    merged, change, weight_in, gain_in, tops, part_router, inverse, columns, banks, wide,
    load_sem, tops_send, tops_recv, hello, send_sem, recv_sem, ring_send, ring_recv, pair_send, pair_recv,
):
    experts, rows, lanes = master.shape
    per_piece = experts * rows // PIECES
    bank_count = banks.shape[0]
    me = lax.axis_index("zero")
    bank = lax.axis_index("bank")
    my_x, my_y = lax.rem(me, SIDE), lax.div(me, SIDE)

    def at(x, y):
        return lax.rem(my_y + y, SIDE) * SIDE + lax.rem(my_x + x, SIDE)

    neighbour = (at(1, 0), at(SIDE - 1, 0), at(0, 1), at(0, SIDE - 1))
    above = lax.rem(bank + 2, bank_count)
    below = lax.rem(bank + bank_count - 2, bank_count)
    partner = bank + 1 - 2 * lax.rem(bank, 2)

    loads = []
    for e in range(experts):
        loads.append(
            (
                pltpu.make_async_copy(master.at[e], merged.at[e], load_sem.at[2 * e]),
                pltpu.make_async_copy(second.at[e], change.at[e], load_sem.at[2 * e + 1]),
            )
        )
        for load in loads[-1]:
            load.start()
    small = (
        pltpu.make_async_copy(weight, weight_in, load_sem.at[2 * experts]),
        pltpu.make_async_copy(gain, gain_in, load_sem.at[2 * experts + 1]),
    )
    for load in small:
        load.start()

    barrier = pltpu.get_barrier_semaphore()
    hops = [min(step, SIDE - step) for step in range(SIDE)]
    offsets = [(x, y) for y in range(SIDE) for x in range(SIDE) if (x, y) != (0, 0)]
    others = [at(x, y) for x, y in sorted(offsets, key=lambda o: -hops[o[0]] - hops[o[1]])]
    for other in others:
        pl.semaphore_signal(barrier, inc=1, device_id={"zero": other}, device_id_type=MESH)
    floor, core = lax.div(bank, 2), lax.rem(bank, 2)
    last = bank_count // 2 - 1

    def greet(semaphore, condition, other):
        @pl.when(condition)
        def _():
            pl.semaphore_signal(semaphore, inc=1, device_id={"bank": other}, device_id_type=MESH)

    def flag(condition):
        return jnp.where(condition, 1, 0)

    greet(barrier, floor < last, above)
    greet(barrier, floor == 0, below)
    greet(barrier, core == 0, partner)

    lane = lax.broadcasted_iota(jnp.int32, (8, lanes), 1)
    groups = rows // 16

    def find_tops(e):
        for load in loads[e]:
            load.wait()

        def body(g, top):
            at_rows = pl.ds(pl.multiple_of(g * 16, 16), 16)
            total = merged[e, at_rows, :] + change[e, at_rows, :].astype(F32)
            merged[e, at_rows, :] = total
            peak = jnp.max(jnp.abs(total), axis=1, keepdims=True)
            top = jnp.where(lane == 2 * g, peak[:8], top)
            return jnp.where(lane == 2 * g + 1, peak[8:], top)

        return lax.fori_loop(0, groups, body, jnp.zeros((8, lanes), F32), unroll=32)

    def remote(part, send_semaphore, recv_semaphore, other):
        return pltpu.make_async_remote_copy(
            part, part, send_semaphore, recv_semaphore, device_id=other, device_id_type=MESH
        )

    def to_all(values, message):
        for other in others:
            remote(values.at[me], tops_send.at[message], tops_recv.at[message], {"zero": other}).start()

        return remote(
            values.at[pl.ds(0, PLANE - 1)], tops_send.at[message], tops_recv.at[message], {"zero": me}
        )

    def divide(e, top):
        columns[e] = top
        inverse[...] = 1.0 / top

        def body(g, carry):
            here = pltpu.roll(inverse[...], lax.rem(lanes - 8 * g, lanes), 1)
            for i in range(4):
                at_rows = pl.ds(pl.multiple_of(g * 64 + 16 * i, 16), 16)
                low = jnp.broadcast_to(here[:, 2 * i : 2 * i + 1], (8, lanes))
                high = jnp.broadcast_to(here[:, 2 * i + 1 : 2 * i + 2], (8, lanes))
                value = merged[e, at_rows, :] * jnp.concatenate([low, high], axis=0)
                to_rows = pl.ds(pl.multiple_of(e * rows + g * 64 + 16 * i, 16), 16)
                slab[me, to_rows, :] = value.astype(BF16)
            return carry

        lax.fori_loop(0, groups // 4, body, 0, unroll=8)

    shared = []
    for e in range(experts):
        tops[e, me] = find_tops(e)
        if e == 0:
            pl.semaphore_wait(barrier, PLANE - 1 + flag(floor > 0) + flag(floor == last) + core)
        shared.append(to_all(tops.at[e], e))
    for load in small:
        load.wait()
    part_router[me] = weight_in[...] * gain_in[...]
    shared.append(to_all(part_router, experts))

    def send(direction, turn):
        piece, (x, y) = ORDER[direction][turn]
        part = slab.at[at(x, y), pl.ds(piece * per_piece, per_piece)]
        remote(part, send_sem, recv_sem.at[turn], {"zero": neighbour[direction]}).start()

    def receive(turn):
        part = slab.at[0, pl.ds(0, 4 * per_piece)]
        remote(part, send_sem, recv_sem.at[turn], {"zero": me}).wait_recv()

    for e in range(experts):
        shared[e].wait_recv()
        divide(e, jnp.max(tops[e], axis=0))
        for turn in range(2 * e, min(2 * e + 2, LEAD)):
            for direction in range(4):
                send(direction, turn)

    def own_bank():
        for j in range(PLANE):
            banks[bank, :, lanes * j : lanes * (j + 1)] = part_router[j]

    def bank_at(shift):
        return lax.rem(bank + bank_count + shift, bank_count)

    ring_copies = []
    pairs = remote(banks.at[pl.ds(0, bank_count // 2)], pair_send, pair_recv, {"bank": bank})

    def ring(step):
        for way, shift, other in ((0, -2, above), (1, 2, below)):
            if step <= bank_count // 4 - way:
                part = banks.at[bank_at(shift * (step - 1))]
                copy = remote(part, ring_send, ring_recv.at[way, step - 1], {"bank": other})
                copy.start()
                ring_copies.append((step, copy))

    def ring_arrived(step):
        for when, copy in ring_copies:
            if when == step:
                copy.wait_recv()

    def pair(shift):
        remote(banks.at[bank_at(shift)], pair_send, pair_recv, {"bank": partner}).start()

    def finish_scale():
        for e in range(experts):
            wide[0:lanes, 0:8] = jnp.transpose(columns[e])
            line = jnp.zeros((8, lanes), F32)
            for q in range(16):
                part = wide[pl.ds(q, 8, stride=16), 0:lanes]
                part = pltpu.roll(part, 8 * q, 1) if q else part
                line = jnp.where((lane >= 8 * q) & (lane < 8 * q + 8), part, line)
            for r in range(8):
                scale_out[e : e + 1, lanes * r : lanes * (r + 1)] = line[r : r + 1, :]

    def finish_router():
        pairs.wait_recv()
        for b in range(bank_count):
            router_out[4 * b : 4 * b + 4, :] = banks[b]

    def ring_step(step):
        def run():
            ring_arrived(step)
            ring(step + 1)
            pair(-2 * step)
            if step < 4:
                pair(2 * step)

        return run

    def say_hello():
        greet(hello, floor > 0, below)
        greet(hello, floor == last, above)
        greet(hello, core == 1, partner)

    def first_step():
        shared[experts].wait_recv()
        own_bank()
        greeted = flag(floor < last) + flag(floor == 0) + 1 - core

        @pl.when(greeted > 0)
        def _():
            pl.semaphore_wait(hello, greeted)

        ring(1)
        pair(0)

    every = TURNS // 10
    extras = {
        0: say_hello,
        1: finish_scale,
        every: first_step,
        2 * every: ring_step(1),
        3 * every: ring_step(2),
        4 * every: ring_step(3),
        5 * every: ring_step(4),
        6 * every: finish_router,
    }

    for turn in range(TURNS):
        receive(turn)
        if turn + LEAD < TURNS:
            for direction in range(4):
                send(direction, turn + LEAD)
        if turn in extras:
            extras[turn]()
    remote(slab.at[pl.ds(0, PLANE - 1)], send_sem, recv_sem.at[0], {"zero": me}).wait_send()
    for copy in shared:
        copy.wait_send()
    remote(
        banks.at[pl.ds(0, bank_count // 2 - 1)], ring_send, ring_recv.at[0, 0], {"bank": bank}
    ).wait_send()
    pairs.wait_send()


def store(slab, scale_in, router_in, final, scale, router, half, sem):
    experts, rows, width = final.shape
    lanes = width // PLANE
    for e in range(experts):
        for j in range(PLANE):
            pltpu.make_async_copy(
                slab.at[j, pl.ds(e * rows, rows)],
                final.at[e, :, pl.ds(j * lanes, lanes)],
                sem.at[0],
            ).start()
    half[...] = router_in[...].astype(BF16)
    small = (
        pltpu.make_async_copy(scale_in, scale, sem.at[1]),
        pltpu.make_async_copy(half, router, sem.at[2]),
    )
    for copy in small:
        copy.start()
    for copy in small:
        copy.wait()
    pltpu.make_async_copy(slab, slab, sem.at[0]).wait()


def shards(master, second, weight, gain):
    experts, rows, lanes = master.shape
    banks = lax.axis_size("bank")
    width = lanes * PLANE
    hbm = pl.BlockSpec(memory_space=pltpu.HBM)
    vmem = pl.BlockSpec(memory_space=pltpu.VMEM)
    dma = pltpu.SemaphoreType.DMA
    values = (master, second, weight.T, gain.reshape(1, lanes))
    slab, scale, router = pl.pallas_call(
        exchange,
        out_shape=(
            pltpu.VMEM((PLANE, experts * rows, lanes), BF16),
            pltpu.VMEM((experts, rows), F32),
            pltpu.VMEM((banks * experts, width), F32),
        ),
        in_specs=[hbm] * 4,
        out_specs=(vmem,) * 3,
        scratch_shapes=[
            pltpu.VMEM((experts, rows, lanes), F32),
            pltpu.VMEM((experts, rows, lanes), BF16),
            pltpu.VMEM((experts, lanes), F32),
            pltpu.VMEM((1, lanes), F32),
            pltpu.VMEM((experts, PLANE, 8, lanes), F32),
            pltpu.VMEM((PLANE, experts, lanes), F32),
            pltpu.VMEM((8, lanes), F32),
            pltpu.VMEM((experts, 8, lanes), F32),
            pltpu.VMEM((banks, experts, width), F32),
            pltpu.VMEM((lanes, lanes), F32),
            dma((2 * experts + 2,)),
            dma((experts + 1,)),
            dma((experts + 1,)),
            pltpu.SemaphoreType.REGULAR,
            dma,
            dma((TURNS,)),
            dma,
            dma((2, banks // 4)),
            dma,
            dma,
        ],
        compiler_params=pltpu.CompilerParams(
            collective_id=0, has_side_effects=True, vmem_limit_bytes=24 << 20
        ),
        name="exchange",
    )(*(pltpu.with_memory_space_constraint(value, pltpu.HBM) for value in values))
    final, scale, router = pl.pallas_call(
        store,
        out_shape=(
            jax.ShapeDtypeStruct((experts, rows, width), BF16),
            jax.ShapeDtypeStruct((experts, rows), F32),
            jax.ShapeDtypeStruct((banks * experts, width), BF16),
        ),
        in_specs=[vmem] * 3,
        out_specs=(hbm,) * 3,
        scratch_shapes=[
            pltpu.VMEM((banks * experts, width), BF16),
            dma((3,)),
        ],
        compiler_params=pltpu.CompilerParams(vmem_limit_bytes=4 << 20),
        name="store",
    )(slab, scale, router)
    return final, scale, router.T


def solution(mesh):
    return jax.shard_map(
        shards,
        mesh=mesh,
        in_specs=(P("bank", None, "zero"), P("bank", None, "zero"), P("zero", "bank"), P("zero")),
        out_specs=(P("bank", None, None), P("bank", None), P()),
        check_vma=False,
    )
```

```python
import jax
import jax.numpy as jnp
from jax import lax
from jax.experimental import pallas as pl
from jax.experimental.pallas import tpu as pltpu
from jax.sharding import PartitionSpec as P

SIDE = 4
PLANE = SIDE * SIDE
EXPERTS = 4
PIECES = 16
LATE = 5
LEAD = 10
MESH = pl.DeviceIdType.MESH
F32 = jnp.float32
BF16 = jnp.bfloat16


def routes(piece, origin, via):
    turned, half = piece % 2, (piece // 2) % 2
    first, second = origin if not turned else origin[::-1]
    if via is None:
        legs = [(0, 3), (1, 3), (2, 1 - half), (3, half)]
    else:
        along = via ^ (2 * turned)
        if along < 2:
            legs = [(2, 1 - half), (3, half)]
            if (along, first, half) in ((0, SIDE - 1, 0), (1, 1, 1)):
                legs.append((along, 2))
        elif (along, second, half) in ((2, SIDE - 1, 0), (3, 1, 1)):
            legs = [(along, 0)]
        else:
            legs = []
    return [(direction ^ (2 * turned), weight) for direction, weight in legs]


STEP = ((-1, 0), (1, 0), (0, -1), (0, 1))


def schedule():
    waiting = [[] for _ in range(4)]
    order = [[] for _ in range(4)]
    events = []
    for piece in range(PIECES):
        for direction, weight in routes(piece, (0, 0), None):
            waiting[direction].append((-weight, 0, piece, (0, 0)))

    def pick(turn):
        limit = (max(0, turn - LATE + 1) + 1) * PIECES // EXPERTS
        now = []
        for depth in range(turn + 1, turn + 1 + LEAD):
            for direction in range(4):
                if len(order[direction]) > depth:
                    continue
                ready = [entry for entry in waiting[direction] if entry[2] < limit or entry[1]]
                if turn < 0:
                    ready = [entry for entry in ready if entry[2] <= depth]
                if ready:
                    best = min(ready)
                    waiting[direction].remove(best)
                    now.append((direction, len(order[direction])))
                    order[direction].append(best[2:])
        events.append(now)

    pick(-1)
    for turn in range((PLANE - 1) * PIECES // 4):
        for direction in range(4):
            piece, origin = order[direction][turn]
            origin = tuple((o + s) % SIDE for o, s in zip(origin, STEP[direction]))
            for onward, weight in routes(piece, origin, direction):
                waiting[onward].append((-weight, turn + 1, piece, origin))
        pick(turn)
    return order, events


ORDER, EVENTS = schedule()
TURNS = (PLANE - 1) * PIECES // 4
assert all(len(lane) == TURNS for lane in ORDER)
assert all(lane[0] == (0, (0, 0)) for lane in ORDER)


def exchange(
    master, second, weight, gain, slab, scale_out, router_out,
    merged, change, weight_in, gain_in, tops, tops_x, tops_y, early, part_router, inverse,
    columns, banks, wide, load_sem, tops_send, tops_recv, axis_send, axis_recv, early_send,
    hello, send_sem, recv_sem, ring_send, ring_recv, pair_send, pair_recv,
):
    experts, rows, lanes = master.shape
    per_piece = experts * rows // PIECES
    bank_count = banks.shape[0]
    me = lax.axis_index("zero")
    bank = lax.axis_index("bank")
    my_x, my_y = lax.rem(me, SIDE), lax.div(me, SIDE)

    def at(x, y):
        return lax.rem(my_y + y, SIDE) * SIDE + lax.rem(my_x + x, SIDE)

    neighbour = (at(1, 0), at(SIDE - 1, 0), at(0, 1), at(0, SIDE - 1))
    above = lax.rem(bank + 2, bank_count)
    below = lax.rem(bank + bank_count - 2, bank_count)
    partner = bank + 1 - 2 * lax.rem(bank, 2)

    loads = []
    for e in range(experts):
        loads.append(
            (
                pltpu.make_async_copy(master.at[e], merged.at[e], load_sem.at[2 * e]),
                pltpu.make_async_copy(second.at[e], change.at[e], load_sem.at[2 * e + 1]),
            )
        )
        for load in loads[-1]:
            load.start()
    small = (
        pltpu.make_async_copy(weight, weight_in, load_sem.at[2 * experts]),
        pltpu.make_async_copy(gain, gain_in, load_sem.at[2 * experts + 1]),
    )
    for load in small:
        load.start()

    barrier = pltpu.get_barrier_semaphore()
    hops = [min(step, SIDE - step) for step in range(SIDE)]
    offsets = [(x, y) for y in range(SIDE) for x in range(SIDE) if (x, y) != (0, 0)]
    others = [at(x, y) for x, y in sorted(offsets, key=lambda o: -hops[o[0]] - hops[o[1]])]
    for other in others:
        pl.semaphore_signal(barrier, inc=1, device_id={"zero": other}, device_id_type=MESH)
    floor, core = lax.div(bank, 2), lax.rem(bank, 2)
    last = bank_count // 2 - 1

    def greet(semaphore, condition, other):
        @pl.when(condition)
        def _():
            pl.semaphore_signal(semaphore, inc=1, device_id={"bank": other}, device_id_type=MESH)

    def flag(condition):
        return jnp.where(condition, 1, 0)

    greet(barrier, floor < last, above)
    greet(barrier, floor == 0, below)
    greet(barrier, core == 0, partner)

    lane = lax.broadcasted_iota(jnp.int32, (8, lanes), 1)
    groups = rows // 16

    def find_tops(e):
        for load in loads[e]:
            load.wait()

        def body(g, top):
            at_rows = pl.ds(pl.multiple_of(g * 16, 16), 16)
            total = merged[e, at_rows, :] + change[e, at_rows, :].astype(F32)
            merged[e, at_rows, :] = total
            peak = jnp.max(jnp.abs(total), axis=1, keepdims=True)
            top = jnp.where(lane == 2 * g, peak[:8], top)
            return jnp.where(lane == 2 * g + 1, peak[8:], top)

        return lax.fori_loop(0, groups, body, jnp.zeros((8, lanes), F32), unroll=32)

    def remote(part, send_semaphore, recv_semaphore, other):
        return pltpu.make_async_remote_copy(
            part, part, send_semaphore, recv_semaphore, device_id=other, device_id_type=MESH
        )

    def to_all(values, message):
        for other in others:
            remote(values.at[me], tops_send.at[message], tops_recv.at[message], {"zero": other}).start()

        return remote(
            values.at[pl.ds(0, PLANE - 1)], tops_send.at[message], tops_recv.at[message], {"zero": me}
        )

    def along(axis, values, mine):
        for step in range(1, SIDE):
            other = at(step, 0) if axis == 0 else at(0, step)
            remote(values.at[mine], axis_send.at[axis], axis_recv.at[axis], {"zero": other}).start()
        return remote(
            values.at[pl.ds(0, SIDE - 1)], axis_send.at[axis], axis_recv.at[axis], {"zero": me}
        )

    def scaled(read, write, count):
        def body(g, carry):
            here = pltpu.roll(inverse[...], lax.rem(lanes - 8 * g, lanes), 1)
            for i in range(4):
                first = pl.multiple_of(g * 64 + 16 * i, 16)
                low = jnp.broadcast_to(here[:, 2 * i : 2 * i + 1], (8, lanes))
                high = jnp.broadcast_to(here[:, 2 * i + 1 : 2 * i + 2], (8, lanes))
                value = read(first) * jnp.concatenate([low, high], axis=0)
                write(first, value.astype(BF16))
            return carry

        lax.fori_loop(0, count // 64, body, 0, unroll=min(8, count // 64))

    def divide(e, top):
        columns[e] = top
        inverse[...] = 1.0 / top

        def write(first, value):
            slab[me, pl.ds(pl.multiple_of(e * rows + first, 16), 16), :] = value

        scaled(lambda first: merged[e, pl.ds(first, 16), :], write, rows)

    def came_from(direction, origin):
        x, y = (o + s for o, s in zip(origin, STEP[direction]))
        return at(x + SIDE, y + SIDE)

    def divide_early():
        for direction in range(4):
            source = came_from(direction, (0, 0))

            def write(first, value):
                slab[source, pl.ds(first, 16), :] = value

            scaled(lambda first: early[direction, pl.ds(first, 16), :], write, per_piece)

    def send(direction, turn):
        piece, (x, y) = ORDER[direction][turn]
        part = slab.at[at(x, y), pl.ds(piece * per_piece, per_piece)]
        remote(part, send_sem, recv_sem.at[turn], {"zero": neighbour[direction]}).start()

    def receive(turn):
        part = slab.at[0, pl.ds(0, 4 * per_piece)]
        remote(part, send_sem, recv_sem.at[turn], {"zero": me}).wait_recv()

    tops[me] = find_tops(0)
    pl.semaphore_wait(barrier, PLANE - 1 + flag(floor > 0) + flag(floor == last) + core)
    shared = [to_all(tops, 0)]
    for direction in range(4):
        pltpu.make_async_remote_copy(
            merged.at[0, pl.ds(0, per_piece)], early.at[direction], early_send, recv_sem.at[0],
            device_id={"zero": neighbour[direction]}, device_id_type=MESH,
        ).start()
    for e in range(1, experts):
        tops_x[my_x, e - 1] = find_tops(e)
    by_axis = [along(0, tops_x, my_x)]
    for load in small:
        load.wait()
    part_router[me] = weight_in[...] * gain_in[...]
    shared.append(to_all(part_router, 1))

    def send_all(events):
        for direction, turn in events:
            if turn:
                send(direction, turn)

    shared[0].wait_recv()
    divide(0, jnp.max(tops[...], axis=0))
    send_all(EVENTS[0])
    all_early = remote(early, early_send, recv_sem.at[0], {"zero": me})
    all_early.wait_recv()
    divide_early()
    send_all(EVENTS[1])
    by_axis[0].wait_recv()
    tops_y[my_y] = jnp.max(tops_x[...], axis=0)
    by_axis.append(along(1, tops_y, my_y))

    def own_bank():
        for j in range(PLANE):
            banks[bank, :, lanes * j : lanes * (j + 1)] = part_router[j]

    def bank_at(shift):
        return lax.rem(bank + bank_count + shift, bank_count)

    ring_copies = []
    pairs = remote(banks.at[pl.ds(0, bank_count // 2)], pair_send, pair_recv, {"bank": bank})

    def ring(step):
        for way, shift, other in ((0, -2, above), (1, 2, below)):
            if step <= bank_count // 4 - way:
                part = banks.at[bank_at(shift * (step - 1))]
                copy = remote(part, ring_send, ring_recv.at[way, step - 1], {"bank": other})
                copy.start()
                ring_copies.append((step, copy))

    def ring_arrived(step):
        for when, copy in ring_copies:
            if when == step:
                copy.wait_recv()

    def pair(shift):
        remote(banks.at[bank_at(shift)], pair_send, pair_recv, {"bank": partner}).start()

    def finish_scale():
        for e in range(experts):
            wide[0:lanes, 0:8] = jnp.transpose(columns[e])
            line = jnp.zeros((8, lanes), F32)
            for q in range(16):
                part = wide[pl.ds(q, 8, stride=16), 0:lanes]
                part = pltpu.roll(part, 8 * q, 1) if q else part
                line = jnp.where((lane >= 8 * q) & (lane < 8 * q + 8), part, line)
            for r in range(8):
                scale_out[e : e + 1, lanes * r : lanes * (r + 1)] = line[r : r + 1, :]

    def finish_router():
        pairs.wait_recv()
        for b in range(bank_count):
            router_out[4 * b : 4 * b + 4, :] = banks[b]

    def ring_step(step):
        def run():
            ring_arrived(step)
            ring(step + 1)
            pair(-2 * step)
            if step < 4:
                pair(2 * step)

        return run

    def say_hello():
        greet(hello, floor > 0, below)
        greet(hello, floor == last, above)
        greet(hello, core == 1, partner)

    def first_step():
        shared[1].wait_recv()
        own_bank()
        greeted = flag(floor < last) + flag(floor == 0) + 1 - core

        @pl.when(greeted > 0)
        def _():
            pl.semaphore_wait(hello, greeted)

        ring(1)
        pair(0)

    def late(e):
        if e == 1:
            by_axis[1].wait_recv()
        divide(e, jnp.max(tops_y[:, e - 1], axis=0))

    every = TURNS // 10
    extras = {
        1: say_hello,
        LATE + 5: finish_scale,
        LATE + 8: first_step,
        4 * every: ring_step(1),
        5 * every: ring_step(2),
        6 * every: ring_step(3),
        7 * every: ring_step(4),
        8 * every: finish_router,
    }

    for turn in range(1, TURNS):
        receive(turn)
        if LATE <= turn < LATE + experts - 1:
            late(turn - LATE + 1)
        send_all(EVENTS[turn + 1])
        if turn in extras:
            extras[turn]()
    turns = slab.reshape(PLANE * SIDE, experts * rows // SIDE, lanes)
    remote(turns.at[pl.ds(0, TURNS - 1)], send_sem, recv_sem.at[0], {"zero": me}).wait_send()
    for copy in [all_early, *shared, *by_axis]:
        copy.wait_send()
    remote(
        banks.at[pl.ds(0, bank_count // 2 - 1)], ring_send, ring_recv.at[0, 0], {"bank": bank}
    ).wait_send()
    pairs.wait_send()


def store(slab, scale_in, router_in, final, scale, router, half, sem):
    experts, rows, width = final.shape
    lanes = width // PLANE
    for e in range(experts):
        for j in range(PLANE):
            pltpu.make_async_copy(
                slab.at[j, pl.ds(e * rows, rows)],
                final.at[e, :, pl.ds(j * lanes, lanes)],
                sem.at[0],
            ).start()
    half[...] = router_in[...].astype(BF16)
    small = (
        pltpu.make_async_copy(scale_in, scale, sem.at[1]),
        pltpu.make_async_copy(half, router, sem.at[2]),
    )
    for copy in small:
        copy.start()
    for copy in small:
        copy.wait()
    pltpu.make_async_copy(slab, slab, sem.at[0]).wait()


def shards(master, second, weight, gain):
    experts, rows, lanes = master.shape
    banks = lax.axis_size("bank")
    width = lanes * PLANE
    hbm = pl.BlockSpec(memory_space=pltpu.HBM)
    vmem = pl.BlockSpec(memory_space=pltpu.VMEM)
    dma = pltpu.SemaphoreType.DMA
    values = (master, second, weight.T, gain.reshape(1, lanes))
    slab, scale, router = pl.pallas_call(
        exchange,
        out_shape=(
            pltpu.VMEM((PLANE, experts * rows, lanes), BF16),
            pltpu.VMEM((experts, rows), F32),
            pltpu.VMEM((banks * experts, width), F32),
        ),
        in_specs=[hbm] * 4,
        out_specs=(vmem,) * 3,
        scratch_shapes=[
            pltpu.VMEM((experts, rows, lanes), F32),
            pltpu.VMEM((experts, rows, lanes), BF16),
            pltpu.VMEM((experts, lanes), F32),
            pltpu.VMEM((1, lanes), F32),
            pltpu.VMEM((PLANE, 8, lanes), F32),
            pltpu.VMEM((SIDE, experts - 1, 8, lanes), F32),
            pltpu.VMEM((SIDE, experts - 1, 8, lanes), F32),
            pltpu.VMEM((4, experts * rows // PIECES, lanes), F32),
            pltpu.VMEM((PLANE, experts, lanes), F32),
            pltpu.VMEM((8, lanes), F32),
            pltpu.VMEM((experts, 8, lanes), F32),
            pltpu.VMEM((banks, experts, width), F32),
            pltpu.VMEM((lanes, lanes), F32),
            dma((2 * experts + 2,)),
            dma((2,)),
            dma((2,)),
            dma((2,)),
            dma((2,)),
            dma,
            pltpu.SemaphoreType.REGULAR,
            dma,
            dma((TURNS,)),
            dma,
            dma((2, banks // 4)),
            dma,
            dma,
        ],
        compiler_params=pltpu.CompilerParams(
            collective_id=0, has_side_effects=True, vmem_limit_bytes=24 << 20
        ),
        name="exchange",
    )(*(pltpu.with_memory_space_constraint(value, pltpu.HBM) for value in values))
    final, scale, router = pl.pallas_call(
        store,
        out_shape=(
            jax.ShapeDtypeStruct((experts, rows, width), BF16),
            jax.ShapeDtypeStruct((experts, rows), F32),
            jax.ShapeDtypeStruct((banks * experts, width), BF16),
        ),
        in_specs=[vmem] * 3,
        out_specs=(hbm,) * 3,
        scratch_shapes=[
            pltpu.VMEM((banks * experts, width), BF16),
            dma((3,)),
        ],
        compiler_params=pltpu.CompilerParams(vmem_limit_bytes=4 << 20),
        name="store",
    )(slab, scale, router)
    return final, scale, router.T


def solution(mesh):
    return jax.shard_map(
        shards,
        mesh=mesh,
        in_specs=(P("bank", None, "zero"), P("bank", None, "zero"), P("zero", "bank"), P("zero")),
        out_specs=(P("bank", None, None), P("bank", None), P()),
        check_vma=False,
    )
```

```python
import jax
import jax.numpy as jnp
from jax import lax
from jax.experimental import pallas as pl
from jax.experimental.pallas import tpu as pltpu
from jax.sharding import PartitionSpec as P

SIDE = 4
PLANE = SIDE * SIDE
EXPERTS = 4
PIECES = 16
LATE = 5
ALONE, SPAN = 8, 2
LEAD = 10
MESH = pl.DeviceIdType.MESH
F32 = jnp.float32
BF16 = jnp.bfloat16


def routes(piece, origin, via):
    turned, half = piece % 2, (piece // 2) % 2
    first, second = origin if not turned else origin[::-1]
    if via is None:
        legs = [(0, 3), (1, 3), (2, 1 - half), (3, half)]
    else:
        along = via ^ (2 * turned)
        if along < 2:
            legs = [(2, 1 - half), (3, half)]
            if (along, first, half) in ((0, SIDE - 1, 0), (1, 1, 1)):
                legs.append((along, 2))
        elif (along, second, half) in ((2, SIDE - 1, 0), (3, 1, 1)):
            legs = [(along, 0)]
        else:
            legs = []
    return [(direction ^ (2 * turned), weight) for direction, weight in legs]


STEP = ((-1, 0), (1, 0), (0, -1), (0, 1))


TURNS = (PLANE - 1) * PIECES // 4
GROUPS = [[turn] for turn in range(ALONE)]
GROUPS += [list(range(turn, turn + SPAN)) for turn in range(ALONE, TURNS, SPAN)]
PLACE = {turn: place for place, group in enumerate(GROUPS) for turn in group}


def schedule():
    waiting = [[] for _ in range(4)]
    order = [[] for _ in range(4)]
    events = []
    for piece in range(PIECES):
        for direction, weight in routes(piece, (0, 0), None):
            waiting[direction].append((-weight, 0, piece, (0, 0)))

    def pick(turn):
        limit = (max(0, turn - LATE + 1) + 1) * PIECES // EXPERTS
        now = []
        for depth in range(turn + 1, turn + 1 + LEAD):
            for direction in range(4):
                if len(order[direction]) > depth:
                    continue
                ready = [entry for entry in waiting[direction] if entry[2] < limit or entry[1]]
                if turn < 0:
                    ready = [entry for entry in ready if entry[2] <= depth]
                if ready:
                    best = min(ready)
                    waiting[direction].remove(best)
                    now.append((direction, len(order[direction])))
                    order[direction].append(best[2:])
        events.append(now)

    pick(-1)
    for group in GROUPS:
        for turn in group:
            for direction in range(4):
                piece, origin = order[direction][turn]
                origin = tuple((o + s) % SIDE for o, s in zip(origin, STEP[direction]))
                for onward, weight in routes(piece, origin, direction):
                    waiting[onward].append((-weight, turn + 1, piece, origin))
        pick(group[-1])
    return order, events


ORDER, EVENTS = schedule()
assert all(len(lane) == TURNS for lane in ORDER)
assert all(lane[0] == (0, (0, 0)) for lane in ORDER)


def exchange(
    master, second, weight, gain, slab, scale_out, router_out,
    merged, change, weight_in, gain_in, tops, tops_x, tops_y, early, part_router, inverse,
    columns, banks, wide, load_sem, tops_send, tops_recv, axis_send, axis_recv, early_send,
    hello, send_sem, recv_sem, ring_send, ring_recv, pair_send, pair_recv,
):
    experts, rows, lanes = master.shape
    per_piece = experts * rows // PIECES
    bank_count = banks.shape[0]
    me = lax.axis_index("zero")
    bank = lax.axis_index("bank")
    my_x, my_y = lax.rem(me, SIDE), lax.div(me, SIDE)

    def at(x, y):
        return lax.rem(my_y + y, SIDE) * SIDE + lax.rem(my_x + x, SIDE)

    neighbour = (at(1, 0), at(SIDE - 1, 0), at(0, 1), at(0, SIDE - 1))
    above = lax.rem(bank + 2, bank_count)
    below = lax.rem(bank + bank_count - 2, bank_count)
    partner = bank + 1 - 2 * lax.rem(bank, 2)

    loads = []
    for e in range(experts):
        loads.append(
            (
                pltpu.make_async_copy(master.at[e], merged.at[e], load_sem.at[2 * e]),
                pltpu.make_async_copy(second.at[e], change.at[e], load_sem.at[2 * e + 1]),
            )
        )
        for load in loads[-1]:
            load.start()
    small = (
        pltpu.make_async_copy(weight, weight_in, load_sem.at[2 * experts]),
        pltpu.make_async_copy(gain, gain_in, load_sem.at[2 * experts + 1]),
    )
    for load in small:
        load.start()

    barrier = pltpu.get_barrier_semaphore()
    hops = [min(step, SIDE - step) for step in range(SIDE)]
    offsets = [(x, y) for y in range(SIDE) for x in range(SIDE) if (x, y) != (0, 0)]
    others = [at(x, y) for x, y in sorted(offsets, key=lambda o: -hops[o[0]] - hops[o[1]])]
    for other in others:
        pl.semaphore_signal(barrier, inc=1, device_id={"zero": other}, device_id_type=MESH)
    floor, core = lax.div(bank, 2), lax.rem(bank, 2)
    last = bank_count // 2 - 1

    def greet(semaphore, condition, other):
        @pl.when(condition)
        def _():
            pl.semaphore_signal(semaphore, inc=1, device_id={"bank": other}, device_id_type=MESH)

    def flag(condition):
        return jnp.where(condition, 1, 0)

    greet(barrier, floor < last, above)
    greet(barrier, floor == 0, below)
    greet(barrier, core == 0, partner)

    lane = lax.broadcasted_iota(jnp.int32, (8, lanes), 1)
    groups = rows // 16

    def find_tops(e):
        for load in loads[e]:
            load.wait()

        def body(g, top):
            at_rows = pl.ds(pl.multiple_of(g * 16, 16), 16)
            total = merged[e, at_rows, :] + change[e, at_rows, :].astype(F32)
            merged[e, at_rows, :] = total
            peak = jnp.max(jnp.abs(total), axis=1, keepdims=True)
            top = jnp.where(lane == 2 * g, peak[:8], top)
            return jnp.where(lane == 2 * g + 1, peak[8:], top)

        return lax.fori_loop(0, groups, body, jnp.zeros((8, lanes), F32), unroll=32)

    def remote(part, send_semaphore, recv_semaphore, other):
        return pltpu.make_async_remote_copy(
            part, part, send_semaphore, recv_semaphore, device_id=other, device_id_type=MESH
        )

    def to_all(values, message):
        for other in others:
            remote(values.at[me], tops_send.at[message], tops_recv.at[message], {"zero": other}).start()

        return remote(
            values.at[pl.ds(0, PLANE - 1)], tops_send.at[message], tops_recv.at[message], {"zero": me}
        )

    def along(axis, values, mine):
        for step in range(1, SIDE):
            other = at(step, 0) if axis == 0 else at(0, step)
            remote(values.at[mine], axis_send.at[axis], axis_recv.at[axis], {"zero": other}).start()
        return remote(
            values.at[pl.ds(0, SIDE - 1)], axis_send.at[axis], axis_recv.at[axis], {"zero": me}
        )

    def scaled(read, write, count):
        def body(g, carry):
            here = pltpu.roll(inverse[...], lax.rem(lanes - 8 * g, lanes), 1)
            for i in range(4):
                first = pl.multiple_of(g * 64 + 16 * i, 16)
                low = jnp.broadcast_to(here[:, 2 * i : 2 * i + 1], (8, lanes))
                high = jnp.broadcast_to(here[:, 2 * i + 1 : 2 * i + 2], (8, lanes))
                value = read(first) * jnp.concatenate([low, high], axis=0)
                write(first, value.astype(BF16))
            return carry

        lax.fori_loop(0, count // 64, body, 0, unroll=min(8, count // 64))

    def divide(e, top):
        columns[e] = top
        inverse[...] = 1.0 / top

        def write(first, value):
            slab[me, pl.ds(pl.multiple_of(e * rows + first, 16), 16), :] = value

        scaled(lambda first: merged[e, pl.ds(first, 16), :], write, rows)

    def came_from(direction, origin):
        x, y = (o + s for o, s in zip(origin, STEP[direction]))
        return at(x + SIDE, y + SIDE)

    def divide_early():
        for direction in range(4):
            source = came_from(direction, (0, 0))

            def write(first, value):
                slab[source, pl.ds(first, 16), :] = value

            scaled(lambda first: early[direction, pl.ds(first, 16), :], write, per_piece)

    def send(direction, turn):
        piece, (x, y) = ORDER[direction][turn]
        part = slab.at[at(x, y), pl.ds(piece * per_piece, per_piece)]
        semaphore = recv_sem.at[PLACE[turn]]
        remote(part, send_sem, semaphore, {"zero": neighbour[direction]}).start()

    def receive(place):
        part = slab.at[0, pl.ds(0, 4 * per_piece * len(GROUPS[place]))]
        remote(part, send_sem, recv_sem.at[place], {"zero": me}).wait_recv()

    tops[me] = find_tops(0)
    pl.semaphore_wait(barrier, PLANE - 1 + flag(floor > 0) + flag(floor == last) + core)
    shared = [to_all(tops, 0)]
    for direction in range(4):
        pltpu.make_async_remote_copy(
            merged.at[0, pl.ds(0, per_piece)], early.at[direction], early_send, recv_sem.at[0],
            device_id={"zero": neighbour[direction]}, device_id_type=MESH,
        ).start()
    for e in range(1, experts):
        tops_x[my_x, e - 1] = find_tops(e)
    by_axis = [along(0, tops_x, my_x)]
    for load in small:
        load.wait()
    part_router[me] = weight_in[...] * gain_in[...]
    shared.append(to_all(part_router, 1))

    def send_all(events):
        for direction, turn in events:
            if turn:
                send(direction, turn)

    shared[0].wait_recv()
    divide(0, jnp.max(tops[...], axis=0))
    send_all(EVENTS[0])
    all_early = remote(early, early_send, recv_sem.at[0], {"zero": me})
    all_early.wait_recv()
    divide_early()
    send_all(EVENTS[1])
    by_axis[0].wait_recv()
    tops_y[my_y] = jnp.max(tops_x[...], axis=0)
    by_axis.append(along(1, tops_y, my_y))

    def own_bank():
        for j in range(PLANE):
            banks[bank, :, lanes * j : lanes * (j + 1)] = part_router[j]

    def bank_at(shift):
        return lax.rem(bank + bank_count + shift, bank_count)

    ring_copies = []
    pairs = remote(banks.at[pl.ds(0, bank_count // 2)], pair_send, pair_recv, {"bank": bank})

    def ring(step):
        for way, shift, other in ((0, -2, above), (1, 2, below)):
            if step <= bank_count // 4 - way:
                part = banks.at[bank_at(shift * (step - 1))]
                copy = remote(part, ring_send, ring_recv.at[way, step - 1], {"bank": other})
                copy.start()
                ring_copies.append((step, copy))

    def ring_arrived(step):
        for when, copy in ring_copies:
            if when == step:
                copy.wait_recv()

    def pair(shift):
        remote(banks.at[bank_at(shift)], pair_send, pair_recv, {"bank": partner}).start()

    def finish_scale():
        for e in range(experts):
            wide[0:lanes, 0:8] = jnp.transpose(columns[e])
            line = jnp.zeros((8, lanes), F32)
            for q in range(16):
                part = wide[pl.ds(q, 8, stride=16), 0:lanes]
                part = pltpu.roll(part, 8 * q, 1) if q else part
                line = jnp.where((lane >= 8 * q) & (lane < 8 * q + 8), part, line)
            for r in range(8):
                scale_out[e : e + 1, lanes * r : lanes * (r + 1)] = line[r : r + 1, :]

    def finish_router():
        pairs.wait_recv()
        for b in range(bank_count):
            router_out[4 * b : 4 * b + 4, :] = banks[b]

    def ring_step(step):
        def run():
            ring_arrived(step)
            ring(step + 1)
            pair(-2 * step)
            if step < 4:
                pair(2 * step)

        return run

    def say_hello():
        greet(hello, floor > 0, below)
        greet(hello, floor == last, above)
        greet(hello, core == 1, partner)

    def first_step():
        shared[1].wait_recv()
        own_bank()
        greeted = flag(floor < last) + flag(floor == 0) + 1 - core

        @pl.when(greeted > 0)
        def _():
            pl.semaphore_wait(hello, greeted)

        ring(1)
        pair(0)

    def late(e):
        if e == 1:
            by_axis[1].wait_recv()
        divide(e, jnp.max(tops_y[:, e - 1], axis=0))

    every = TURNS // 10
    extras = {
        1: say_hello,
        LATE + 5: finish_scale,
        LATE + 8: first_step,
        4 * every: ring_step(1),
        5 * every: ring_step(2),
        6 * every: ring_step(3),
        7 * every: ring_step(4),
        8 * every: finish_router,
    }

    for place, group in list(enumerate(GROUPS))[1:]:
        receive(place)
        for turn in group:
            if LATE <= turn < LATE + experts - 1:
                late(turn - LATE + 1)
        send_all(EVENTS[place + 1])
        for turn in group:
            if turn in extras:
                extras[turn]()
    turns = slab.reshape(PLANE * SIDE, experts * rows // SIDE, lanes)
    remote(turns.at[pl.ds(0, TURNS - 1)], send_sem, recv_sem.at[0], {"zero": me}).wait_send()
    for copy in [all_early, *shared, *by_axis]:
        copy.wait_send()
    remote(
        banks.at[pl.ds(0, bank_count // 2 - 1)], ring_send, ring_recv.at[0, 0], {"bank": bank}
    ).wait_send()
    pairs.wait_send()


def store(slab, scale_in, router_in, final, scale, router, half, sem):
    experts, rows, width = final.shape
    lanes = width // PLANE
    for e in range(experts):
        for j in range(PLANE):
            pltpu.make_async_copy(
                slab.at[j, pl.ds(e * rows, rows)],
                final.at[e, :, pl.ds(j * lanes, lanes)],
                sem.at[0],
            ).start()
    half[...] = router_in[...].astype(BF16)
    small = (
        pltpu.make_async_copy(scale_in, scale, sem.at[1]),
        pltpu.make_async_copy(half, router, sem.at[2]),
    )
    for copy in small:
        copy.start()
    for copy in small:
        copy.wait()
    pltpu.make_async_copy(slab, slab, sem.at[0]).wait()


def shards(master, second, weight, gain):
    experts, rows, lanes = master.shape
    banks = lax.axis_size("bank")
    width = lanes * PLANE
    hbm = pl.BlockSpec(memory_space=pltpu.HBM)
    vmem = pl.BlockSpec(memory_space=pltpu.VMEM)
    dma = pltpu.SemaphoreType.DMA
    values = (master, second, weight.T, gain.reshape(1, lanes))
    slab, scale, router = pl.pallas_call(
        exchange,
        out_shape=(
            pltpu.VMEM((PLANE, experts * rows, lanes), BF16),
            pltpu.VMEM((experts, rows), F32),
            pltpu.VMEM((banks * experts, width), F32),
        ),
        in_specs=[hbm] * 4,
        out_specs=(vmem,) * 3,
        scratch_shapes=[
            pltpu.VMEM((experts, rows, lanes), F32),
            pltpu.VMEM((experts, rows, lanes), BF16),
            pltpu.VMEM((experts, lanes), F32),
            pltpu.VMEM((1, lanes), F32),
            pltpu.VMEM((PLANE, 8, lanes), F32),
            pltpu.VMEM((SIDE, experts - 1, 8, lanes), F32),
            pltpu.VMEM((SIDE, experts - 1, 8, lanes), F32),
            pltpu.VMEM((4, experts * rows // PIECES, lanes), F32),
            pltpu.VMEM((PLANE, experts, lanes), F32),
            pltpu.VMEM((8, lanes), F32),
            pltpu.VMEM((experts, 8, lanes), F32),
            pltpu.VMEM((banks, experts, width), F32),
            pltpu.VMEM((lanes, lanes), F32),
            dma((2 * experts + 2,)),
            dma((2,)),
            dma((2,)),
            dma((2,)),
            dma((2,)),
            dma,
            pltpu.SemaphoreType.REGULAR,
            dma,
            dma((len(GROUPS),)),
            dma,
            dma((2, banks // 4)),
            dma,
            dma,
        ],
        compiler_params=pltpu.CompilerParams(
            collective_id=0, has_side_effects=True, vmem_limit_bytes=24 << 20
        ),
        name="exchange",
    )(*(pltpu.with_memory_space_constraint(value, pltpu.HBM) for value in values))
    final, scale, router = pl.pallas_call(
        store,
        out_shape=(
            jax.ShapeDtypeStruct((experts, rows, width), BF16),
            jax.ShapeDtypeStruct((experts, rows), F32),
            jax.ShapeDtypeStruct((banks * experts, width), BF16),
        ),
        in_specs=[vmem] * 3,
        out_specs=(hbm,) * 3,
        scratch_shapes=[
            pltpu.VMEM((banks * experts, width), BF16),
            dma((3,)),
        ],
        compiler_params=pltpu.CompilerParams(vmem_limit_bytes=4 << 20),
        name="store",
    )(slab, scale, router)
    return final, scale, router.T


def solution(mesh):
    return jax.shard_map(
        shards,
        mesh=mesh,
        in_specs=(P("bank", None, "zero"), P("bank", None, "zero"), P("zero", "bank"), P("zero")),
        out_specs=(P("bank", None, None), P("bank", None), P()),
        check_vma=False,
    )
```
